32 devices in a mesh: row: 4 (over x, core), col: 8 (over z, y).
Axes of the slice: x: 2, y: 2, z: 4, core: 2. Of those that a mesh axis runs over, the one named last changes fastest.
Arguments:
- right_sides: bfloat16 [1024, 64, 128], P(('row', 'col')), may hold values from -7 to 7
- weights_fine: bfloat16 [1024, 3, 128, 128], P(('row', 'col')), may hold values from 0 to 2
- columns_fine: int32 [1024, 3], P(('row', 'col')), may hold values from 0 to 1023, as said below
- degree_fine: float32 [1024, 128], P(('row', 'col')), may hold values from 0.05 to 0.5
- owners_fine: int32 [1024, 128], P(('row', 'col')), may hold values from 0 to 31, as said below
- slots_fine: int32 [1024, 128], P(('row', 'col')), may hold values from 0 to 1023
- weights_second: bfloat16 [256, 3, 128, 128], P(('row', 'col')), may hold values from 0 to 8
- columns_second: int32 [256, 3], P(('row', 'col')), may hold values from 0 to 255, as said below
- degree_second: float32 [256, 128], P(('row', 'col')), may hold values from 0.2 to 2
- owners_second: int32 [256, 128], P(('row', 'col')), may hold values from 0 to 31, as said below
- slots_second: int32 [256, 128], P(('row', 'col')), may hold values from 0 to 255
- weights_third: bfloat16 [64, 3, 128, 128], P(('row', 'col')), may hold values from 0 to 32
- columns_third: int32 [64, 3], P(('row', 'col')), may hold values from 0 to 63, as said below
- degree_third: float32 [64, 128], P(('row', 'col')), may hold values from 0.8 to 8
- owners_third: int32 [64, 128], P(('row', 'col')), may hold values from 0 to 31, as said below
- slots_third: int32 [64, 128], P(('row', 'col')), may hold values from 0 to 127
- coarse_inverse: bfloat16 [4096, 1024], P(('row', 'col')), may hold values from -1 to 1, as said below
Outputs:
- solution: float32 [1024, 64, 128], P(('row', 'col'))
The draws below stay inside these ranges and needn't reach their ends.
Inputs may be any that keep to these rules, and one draw needn't show every extreme that they name: `columns_fine`: every entry lies within 2 blocks of its own row block's index, on the same level. `columns_second`: every entry lies within 2 blocks of its own row block's index, on the same level. `columns_third`: every entry lies within 2 blocks of its own row block's index, on the same level. `owners_fine`: each entry is the device holding the vertex or the one just before or after it in device order. `owners_second`: each entry is the device holding the vertex or the one just before or after it in device order. `owners_third`: each entry is the device holding the vertex or the one just before or after it in device order. `coarse_inverse`: each row group's block is symmetric.
All inputs are finite; a program needn't handle non-finite values.
Results may differ from the reference program's by a relative error of at most 0.0003.
Values may be sent and summed in bfloat16 or wider, within the bound.
A program may use at most 64 MiB of HBM per device.

```python
import math
import jax
import jax.numpy as jnp
from jax import lax

RHS_COUNT = 64
BS = 128
K = 3
HB = 2
SWEEPS = 2
NB2 = 2
NB1 = 8
NB0 = 32
C3 = 128
M3 = 1024
N_ROW = 4
DEVICES = 32


def arrange_columns(drawn, blocks_here):
    total = blocks_here * DEVICES
    spread = 2 * HB + 1
    scores = drawn * spread + jnp.arange(spread, dtype=jnp.int32)[None, :]
    chosen = jnp.argsort(scores, axis=1)[:, :K].astype(jnp.int32) - HB
    rows_here = jnp.arange(total, dtype=jnp.int32)[:, None]
    target = rows_here + chosen
    outside = (target < 0) | (target >= total)
    return jnp.where(outside, rows_here - chosen, target).astype(jnp.int32)


def arrange_owners(drawn, blocks_here):
    total = blocks_here * DEVICES
    device = (jnp.arange(total, dtype=jnp.int32) // blocks_here)[:, None]
    moved = jnp.where(drawn == 6, -1, jnp.where(drawn == 7, 1, 0))
    return jnp.clip(device + moved, 0, DEVICES - 1).astype(jnp.int32)


def draw_right_sides(key, part):
    total_blocks = NB0 * DEVICES
    vertex = (jnp.arange(total_blocks, dtype=jnp.float32)[:, None, None] * BS + jnp.arange(BS, dtype=jnp.float32)[None, None, :]) / (total_blocks * BS * 1.0)
    frequency = jax.random.randint(jax.random.fold_in(key, 41), (RHS_COUNT,), 1, 4).astype(jnp.float32)
    phase = jax.random.uniform(jax.random.fold_in(key, 42), (RHS_COUNT,), jnp.float32, -3.14159, 3.14159)
    amplitude = jax.random.uniform(jax.random.fold_in(key, 43), (RHS_COUNT,), jnp.float32, 0.25, 0.5)
    wave = jnp.sin(6.283185 * frequency[None, :, None] * vertex + phase[None, :, None])
    shape = (total_blocks, RHS_COUNT, BS)
    flips = jax.random.randint(jax.random.fold_in(key, 45), (RHS_COUNT,), 0, 2)
    signs = jnp.where(flips == 0, -1.0, 1.0).astype(jnp.float32)
    smooth = (signs * amplitude)[None, :, None] * wave
    rough = jnp.clip(jax.random.normal(jax.random.fold_in(key, 44), shape, jnp.float32), -6.0, 6.0)
    return (smooth + rough).astype(jnp.bfloat16)


def draw_columns_fine(key, part):
    drawn = jax.random.randint(jax.random.fold_in(key, 11), (NB0 * DEVICES, 2 * HB + 1), 0, 1 << 20)
    return arrange_columns(drawn, NB0)


def draw_columns_second(key, part):
    drawn = jax.random.randint(jax.random.fold_in(key, 12), (NB1 * DEVICES, 2 * HB + 1), 0, 1 << 20)
    return arrange_columns(drawn, NB1)


def draw_columns_third(key, part):
    drawn = jax.random.randint(jax.random.fold_in(key, 13), (NB2 * DEVICES, 2 * HB + 1), 0, 1 << 20)
    return arrange_columns(drawn, NB2)


def draw_owners_fine(key, part):
    drawn = jax.random.randint(jax.random.fold_in(key, 21), (NB0 * DEVICES, BS), 0, 8)
    return arrange_owners(drawn, NB0)


def draw_owners_second(key, part):
    drawn = jax.random.randint(jax.random.fold_in(key, 22), (NB1 * DEVICES, BS), 0, 8)
    return arrange_owners(drawn, NB1)


def draw_owners_third(key, part):
    drawn = jax.random.randint(jax.random.fold_in(key, 23), (NB2 * DEVICES, BS), 0, 8)
    return arrange_owners(drawn, NB2)


def draw_coarse_inverse(key, part):
    groups = DEVICES * C3 // M3
    inner = jax.random.fold_in(key, 31)
    raw = jnp.clip(jax.random.normal(inner, (groups, M3, M3), jnp.float32), -3.0, 3.0)
    symmetric = 0.5 * (raw + jnp.transpose(raw, (0, 2, 1))) * (0.025 / jnp.sqrt(M3 * 1.0))
    matrix = symmetric + 0.05 * jnp.eye(M3, dtype=jnp.float32)[None, :, :]
    return matrix.reshape(groups * M3, M3).astype(jnp.bfloat16)


def place_ends(values, rng, smallest, top_value):
    extent = values.shape
    index_at = [jax.random.randint(jax.random.fold_in(rng, axis), (), 0, extent[axis]) for axis in range(len(extent))]
    values = values.at[tuple(index_at)].set(smallest)
    longest = extent.index(max(extent))
    index_at[longest] = (index_at[longest] + 1) % extent[longest]
    return values.at[tuple(index_at)].set(top_value)


def block_levels(key, extent, pieces, least, largest):
    loudness = 1.0
    for dim, parts in pieces:
        draws = jax.random.uniform(jax.random.fold_in(jax.random.fold_in(key, 6), dim), (parts,), jnp.float32, least / len(pieces), largest / len(pieces))
        loudness = loudness * jnp.repeat(jnp.exp(draws), extent[dim] // parts).reshape((-1,) + (1,) * (len(extent) - 1 - dim))
    return loudness


def setup_inputs(seed: int = 0) -> dict:
    keys = jax.random.split(jax.random.key(seed), 18)
    right_sides = draw_right_sides(jax.random.fold_in(keys[17], 71), 0)
    weights_fine = jnp.clip(2.0 * jax.random.uniform(keys[1], (NB0 * DEVICES, K, BS, BS), jnp.float32) ** block_levels(keys[1], (NB0 * DEVICES, K, BS, BS), ((0, 32),), -0.2, 0.2), 0.0, 2.0).astype(jnp.bfloat16)
    columns_fine = draw_columns_fine(jax.random.fold_in(keys[17], 71), 0)
    degree_fine = jnp.clip(jnp.exp(math.log(0.5) - 2.3025851 * jax.random.uniform(keys[3], (NB0 * DEVICES, BS), jnp.float32) ** block_levels(keys[3], (NB0 * DEVICES, BS), ((0, 32),), -0.2, 0.2)), 0.05, 0.5)
    owners_fine = draw_owners_fine(jax.random.fold_in(keys[17], 71), 0)
    slots_fine = place_ends(jax.random.randint(keys[5], (NB0 * DEVICES, BS), 0, NB1 * BS), jax.random.fold_in(keys[5], 1), 0, (NB1 * BS) - 1).astype(jnp.int32)
    weights_second = jnp.clip(8.0 * jax.random.uniform(keys[6], (NB1 * DEVICES, K, BS, BS), jnp.float32) ** block_levels(keys[6], (NB1 * DEVICES, K, BS, BS), ((0, 32),), -0.2, 0.2), 0.0, 8.0).astype(jnp.bfloat16)
    columns_second = draw_columns_second(jax.random.fold_in(keys[17], 71), 0)
    degree_second = jnp.clip(jnp.exp(math.log(2.0) - 2.3025851 * jax.random.uniform(keys[8], (NB1 * DEVICES, BS), jnp.float32) ** block_levels(keys[8], (NB1 * DEVICES, BS), ((0, 32),), -0.2, 0.2)), 0.2, 2.0)
    owners_second = draw_owners_second(jax.random.fold_in(keys[17], 71), 0)
    slots_second = place_ends(jax.random.randint(keys[10], (NB1 * DEVICES, BS), 0, NB2 * BS), jax.random.fold_in(keys[10], 1), 0, (NB2 * BS) - 1).astype(jnp.int32)
    weights_third = jnp.clip(32.0 * jax.random.uniform(keys[11], (NB2 * DEVICES, K, BS, BS), jnp.float32) ** block_levels(keys[11], (NB2 * DEVICES, K, BS, BS), ((0, 32),), -0.2, 0.2), 0.0, 32.0).astype(jnp.bfloat16)
    columns_third = draw_columns_third(jax.random.fold_in(keys[17], 71), 0)
    degree_third = jnp.clip(jnp.exp(math.log(8.0) - 2.3025851 * jax.random.uniform(keys[13], (NB2 * DEVICES, BS), jnp.float32) ** block_levels(keys[13], (NB2 * DEVICES, BS), ((0, 32),), -0.2, 0.2)), 0.8, 8.0)
    owners_third = draw_owners_third(jax.random.fold_in(keys[17], 71), 0)
    slots_third = place_ends(jax.random.randint(keys[15], (NB2 * DEVICES, BS), 0, C3), jax.random.fold_in(keys[15], 1), 0, C3 - 1).astype(jnp.int32)
    coarse_inverse = draw_coarse_inverse(jax.random.fold_in(keys[17], 71), 0)
    return dict(right_sides=right_sides, weights_fine=weights_fine, columns_fine=columns_fine, degree_fine=degree_fine, owners_fine=owners_fine, slots_fine=slots_fine, weights_second=weights_second, columns_second=columns_second, degree_second=degree_second, owners_second=owners_second, slots_second=slots_second, weights_third=weights_third, columns_third=columns_third, degree_third=degree_third, owners_third=owners_third, slots_third=slots_third, coarse_inverse=coarse_inverse)


damping = 0.8


def gather_rows(blocks):
    return jnp.transpose(blocks, (0, 2, 1)).reshape(-1, RHS_COUNT)


def make_blocks(rows_data):
    return jnp.transpose(rows_data.reshape(-1, BS, RHS_COUNT), (0, 2, 1))


def complete_diagonal_entries(weights, shift):
    return shift + jnp.sum(weights, axis=(1, 2), dtype=jnp.float32) / (K * BS)


def apply_operator(current_iterate, weights, columns, degree):
    total = current_iterate.shape[0]
    per_device = total // DEVICES
    rounded = lax.optimization_barrier(current_iterate.astype(jnp.bfloat16))
    widened = rounded.astype(jnp.float32)
    shaped_weights = weights.reshape(DEVICES, per_device, K, BS, BS)
    shaped_columns = columns.reshape(DEVICES, per_device, K)

    def per_block(packed):
        block_weights, block_columns = packed
        picked = widened[block_columns]
        return jnp.einsum("nkrb,nkbc->nrc", picked, block_weights.astype(jnp.float32), precision=lax.Precision.HIGHEST)

    product = lax.map(per_block, (shaped_weights, shaped_columns)).reshape(total, RHS_COUNT, BS)
    return degree[:, None, :] * current_iterate - product / (K * BS)


def reference(right_sides, weights_fine, columns_fine, degree_fine, owners_fine, slots_fine, weights_second, columns_second, degree_second, owners_second, slots_second, weights_third, columns_third, degree_third, owners_third, slots_third, coarse_inverse):
    levels = [(weights_fine, columns_fine, complete_diagonal_entries(weights_fine, degree_fine), owners_fine, slots_fine, NB1 * BS),
              (weights_second, columns_second, complete_diagonal_entries(weights_second, degree_second), owners_second, slots_second, NB2 * BS),
              (weights_third, columns_third, complete_diagonal_entries(weights_third, degree_third), owners_third, slots_third, C3)]
    source = right_sides.astype(jnp.float32)
    stored = []
    coarse_rows = None
    for position in range(3):
        weights, columns, degree, aggregate_owners, slots, coarse_count = levels[position]
        scale = degree[:, None, :]
        current_iterate = damping * source / scale
        for repeat in range(SWEEPS - 1):
            current_iterate = current_iterate + damping * (source - apply_operator(current_iterate, weights, columns, degree)) / scale
        residual = source - apply_operator(current_iterate, weights, columns, degree)
        stored.append((current_iterate, source))
        targets = (aggregate_owners * coarse_count + slots).reshape(-1).astype(jnp.int32)
        coarse_rows = jax.ops.segment_sum(gather_rows(residual), targets, num_segments=DEVICES * coarse_count)
        if position < 2:
            source = make_blocks(coarse_rows)
    aggregated_values = lax.optimization_barrier(coarse_rows.astype(jnp.bfloat16)).astype(jnp.float32).reshape(N_ROW, M3, RHS_COUNT)
    inverse_matrix = coarse_inverse.astype(jnp.float32).reshape(N_ROW, M3, M3)
    coarse_correction_rows = jnp.einsum("dut,dtx->dux", inverse_matrix, aggregated_values, precision=lax.Precision.HIGHEST).reshape(-1, RHS_COUNT)
    current_iterate = None
    for position in (2, 1, 0):
        weights, columns, degree, aggregate_owners, slots, coarse_count = levels[position]
        current_iterate, source = stored[position]
        targets = (aggregate_owners * coarse_count + slots).reshape(-1).astype(jnp.int32)
        current_iterate = current_iterate + make_blocks(coarse_correction_rows[targets])
        scale = degree[:, None, :]
        for repeat in range(SWEEPS):
            current_iterate = current_iterate + damping * (source - apply_operator(current_iterate, weights, columns, degree)) / scale
        coarse_correction_rows = gather_rows(current_iterate)
    return current_iterate
```

```python
import functools

import jax
import jax.numpy as jnp
from jax import lax
from jax.experimental import pallas as pl
from jax.experimental.pallas import tpu as pltpu
from jax.sharding import PartitionSpec as P

F32 = jnp.float32
BF16 = jnp.bfloat16
MESH = pl.DeviceIdType.MESH
DAMPING = 0.8
SPLIT_OWN = False


def loop(low, high, body, unroll=4):
    count = high - low
    if count <= 0:
        return
    while count % unroll:
        unroll -= 1

    if count == unroll:
        for inner in range(count):
            body(low + inner)
        return

    def step(outer, carry):
        for inner in range(unroll):
            body(low + outer * unroll + inner)
        return carry

    lax.fori_loop(0, count // unroll, step, 0)


class Level:
    def __init__(self, blocks, coarse, rhs_count, bs, k, ref, hbm, columns, ops):
        self.n, self.t, self.r, self.bs, self.k = blocks, coarse, rhs_count, bs, k
        self.ref, self.hbm, self.columns, self.ops = ref, hbm, columns, ops
        self.single = blocks < 4
        self.base = ops.me * blocks
        self.scale = 1.0 / (k * bs)

    def edges(self):
        n = self.n
        if self.single:
            return list(range(n))
        return [0, 1, n - 2, n - 1]

    def inner(self):
        return (0, 0) if self.single else (2, self.n - 2)

    def make_diagonal(self, b):
        w = self.ref["w"][b]
        total = jnp.dot(jnp.ones((8, w.shape[0]), BF16), w, preferred_element_type=F32)
        degree = self.ref["deg"][pl.ds(b, 1), :]
        g = degree + total * self.scale
        self.ref["g"][b] = g
        self.ref["gi"][b] = DAMPING / g

    def row(self, name, b):
        value = self.ref[name][b, 0:1, :]
        return jnp.broadcast_to(value, (self.r, self.bs))

    def f(self, b):
        return self.ref["f"][b].astype(F32)

    def product(self, i, b, where):
        if where == "inner":
            buf, offset = self.ref["vb"].at[i], self.base
        elif where == "low":
            buf, offset = self.ref[f"lo{i}"], self.base - 2
        else:
            buf, offset = self.ref[f"hi{i}"], self.base + self.n - 4
        top = buf.shape[0] - 1
        picked = [
            buf[jnp.clip(self.columns[b, k] - offset, 0, top)] for k in range(self.k)
        ]
        left = jnp.concatenate(picked, axis=1)
        return jnp.dot(left, self.ref["w"][b], preferred_element_type=F32) * self.scale

    def halo_copies(self, i):
        n, ops, vb = self.n, self.ops, self.ref["vb"].at[i]
        if self.single:
            low_dst, high_dst = self.ref[f"lo{i}"].at[0:2], self.ref[f"lo{i}"].at[4:6]
        else:
            low_dst, high_dst = self.ref[f"lo{i}"].at[0:2], self.ref[f"hi{i}"].at[4:6]
        return ops.pair(vb.at[n - 2 : n], low_dst, vb.at[0:2], high_dst, self.ref["sem"] + i)

    def fill_edges(self, i):
        n = self.n
        if self.single:
            self.ref[f"lo{i}"][2:4] = self.ref["vb"][i, 0:2]
        else:
            self.ref[f"lo{i}"][2:6] = self.ref["vb"][i, 0:4]
            self.ref[f"hi{i}"][0:4] = self.ref["vb"][i, n - 4 : n]

    def run_edges(self, body):
        for b in self.edges():
            body(b, "low" if b < 2 else "high")

    def apply(self, i, body):
        loop(*self.inner(), lambda b: body(b, "inner"))
        self.fill_edges(i)
        self.ops.wait(self.halo_copies(i))
        self.run_edges(body)

    def start_block(self, b):
        self.ref["vb"][0, b] = (self.row("gi", b) * self.f(b)).astype(BF16)

    def first_sweep(self, b, where):
        f, gi = self.f(b), self.row("gi", b)
        x0 = gi * f
        x = (1.0 - DAMPING) * x0 + gi * (f + self.product(0, b, where))
        self.ref["x"][b] = x
        self.ref["vb"][1, b] = x.astype(BF16)

    def residual(self, b, where):
        res = self.f(b) - self.row("g", b) * self.ref["x"][b] + self.product(1, b, where)
        rel = self.owner(b)
        columns = pl.ds(pl.multiple_of(b * self.bs, self.bs), self.bs)
        rows = self.r
        high = res.astype(BF16)
        zero = jnp.zeros_like(res)
        out = self.ref["res"]
        out[0:rows, columns] = jnp.where(rel < 0, res, zero).astype(BF16)
        out[rows : 2 * rows, columns] = jnp.where(rel > 0, res, zero).astype(BF16)
        own = jnp.where(rel == 0, res, zero)
        high = own.astype(BF16)
        out[2 * rows : 3 * rows, columns] = high
        if SPLIT_OWN:
            out[3 * rows : 4 * rows, columns] = (own - high.astype(F32)).astype(BF16)

    def owner(self, b):
        value = self.ref["own"][pl.ds(b, 1), :] - self.ops.me
        return jnp.broadcast_to(value, (self.r, self.bs))

    def make_onehot(self, b):
        columns = pl.ds(pl.multiple_of(b * self.bs, self.bs), self.bs)
        slots = jnp.broadcast_to(self.ref["slot"][pl.ds(b, 1), :], (self.t, self.bs))
        index = lax.broadcasted_iota(jnp.int32, (self.t, self.bs), 0)
        self.ref["oh"][:, columns] = jnp.where(index == slots, 1.0, 0.0).astype(BF16)

    def restricted(self, rows, put):
        tile = min(self.t, 256)

        def body(j):
            at = pl.ds(pl.multiple_of(j * tile, tile), tile)
            put(
                at,
                lax.dot_general(
                    self.ref["res"][rows, :],
                    self.ref["oh"][at, :],
                    (((1,), (1,)), ((), ())),
                    preferred_element_type=F32,
                ),
            )

        loop(0, self.t // tile, body, 1)

    def restrict_copies(self):
        out, got = self.ref["rout"], self.ref["rin"]
        return self.ops.pair(out.at[1], got.at[0], out.at[0], got.at[1], self.ref["sem"] + 4)

    def restrict(self, into):
        r = self.r

        def put_out(at, value):
            self.ref["rout"][0, :, at] = value[0:r].astype(BF16)
            self.ref["rout"][1, :, at] = value[r : 2 * r].astype(BF16)

        self.restricted(slice(0, 2 * r), put_out)
        copies = self.restrict_copies()
        self.ops.start(copies)

        def put_own(at, value):
            if SPLIT_OWN:
                value = value[0:r] + value[r : 2 * r]
            self.ref["rown"][:, at] = value

        self.restricted(slice(2 * r, (4 if SPLIT_OWN else 3) * r), put_own)
        self.ops.wait(copies)
        for block in range(self.t // self.bs):
            at = slice(block * self.bs, (block + 1) * self.bs)
            into(
                block,
                self.ref["rown"][:, at]
                + self.ref["rin"][0, :, at].astype(F32)
                + self.ref["rin"][1, :, at].astype(F32),
            )

    def down(self, into, while_first=None, while_second=None):
        self.ops.start(self.halo_copies(0))
        loop(*self.inner(), self.start_block)
        if while_first is not None:
            while_first()
        self.apply(0, self.first_sweep)
        self.ops.start(self.halo_copies(1))
        if while_second is not None:
            while_second()
        self.apply(1, self.residual)
        self.restrict(into)

    def prolong_copies(self):
        out, got = self.ref["uout"], self.ref["uin"]
        return self.ops.pair(out, got.at[0], out, got.at[1], self.ref["sem"] + 5)

    def pair_columns(self, pair):
        return pl.ds(pl.multiple_of(pair * 2 * self.bs, 2 * self.bs), 2 * self.bs)

    def add_own(self, pair):
        value = jnp.dot(
            self.ref["uout"][...], self.ref["oh"][:, self.pair_columns(pair)],
            preferred_element_type=F32,
        )
        for half in range(2):
            b = 2 * pair + half
            part = value[:, half * self.bs : (half + 1) * self.bs]
            self.ref["x"][b] = self.ref["x"][b] + jnp.where(self.owner(b) == 0, part, 0.0)

    def add_others(self, pair):
        left = jnp.concatenate([self.ref["uin"][0], self.ref["uin"][1]], axis=0)
        value = jnp.dot(
            left, self.ref["oh"][:, self.pair_columns(pair)], preferred_element_type=F32
        )
        for half in range(2):
            b = 2 * pair + half
            at = slice(half * self.bs, (half + 1) * self.bs)
            rel = self.owner(b)
            x = self.ref["x"][b]
            x = x + jnp.where(rel < 0, value[0 : self.r, at], 0.0)
            x = x + jnp.where(rel > 0, value[self.r : 2 * self.r, at], 0.0)
            self.ref["x"][b] = x
            self.ref["vb"][2, b] = x.astype(BF16)

    def sweep(self, i, last, out=None):
        def body(b, where):
            gi = self.row("gi", b)
            x = (1.0 - DAMPING) * self.ref["x"][b] + gi * (self.f(b) + self.product(i, b, where))
            self.ref["x"][b] = x
            if not last:
                self.ref["vb"][i + 1, b] = x.astype(BF16)
            elif out is not None:
                out(b, x)

        return body

    def up(self, out=None):
        copies = self.prolong_copies()
        self.ops.start(copies)
        pairs = self.n // 2
        loop(0, pairs, self.add_own, 2)
        self.ops.wait(copies)
        self.add_others(0)
        if not self.single:
            self.add_others(pairs - 1)
        self.ops.start(self.halo_copies(2))
        if not self.single:
            loop(1, pairs - 1, self.add_others, 2)
        self.apply(2, self.sweep(2, False))
        self.ops.start(self.halo_copies(3))
        self.apply(3, self.sweep(3, True, out))

    def drain(self):
        for i in range(4):
            self.ops.drain(self.halo_copies(i))
        self.ops.drain(self.restrict_copies())
        self.ops.drain(self.prolong_copies())

    def clear_ends(self):
        for name, first, last in (("rin", 0, 1), ("uin", 0, 1)):
            ref = self.ref[name]

            @pl.when(self.ops.me == 0)
            def _():
                ref[first] = jnp.zeros(ref.shape[1:], ref.dtype)

            @pl.when(self.ops.me == self.ops.total - 1)
            def _():
                ref[last] = jnp.zeros(ref.shape[1:], ref.dtype)


class Ops:
    def __init__(self, send, recv):
        self.send, self.recv = send, recv
        self.rows, self.cols = lax.axis_size("row"), lax.axis_size("col")
        self.total = self.rows * self.cols
        self.row, self.col = lax.axis_index("row"), lax.axis_index("col")
        self.me = self.row * self.cols + self.col
        right = jnp.minimum(self.me + 1, self.total - 1)
        left = jnp.maximum(self.me - 1, 0)
        self.right = (right // self.cols, right % self.cols)
        self.left = (left // self.cols, left % self.cols)
        self.has_right = self.me < self.total - 1
        self.has_left = self.me > 0

    def pair(self, to_right, at_right, to_left, at_left, slot):
        first = pltpu.make_async_remote_copy(
            to_right, at_right, self.send.at[slot, 0], self.recv.at[slot, 0],
            device_id=self.right, device_id_type=MESH,
        )
        second = pltpu.make_async_remote_copy(
            to_left, at_left, self.send.at[slot, 1], self.recv.at[slot, 1],
            device_id=self.left, device_id_type=MESH,
        )
        return first, second

    def start(self, copies):
        pl.when(self.has_right)(lambda: copies[0].start())
        pl.when(self.has_left)(lambda: copies[1].start())

    def wait(self, copies):
        pl.when(self.has_left)(lambda: copies[0].wait_recv())
        pl.when(self.has_right)(lambda: copies[1].wait_recv())

    def drain(self, copies):
        pl.when(self.has_right)(lambda: copies[0].wait_send())
        pl.when(self.has_left)(lambda: copies[1].wait_send())


LEVEL_HBM = ("w", "deg", "own", "slot")
LEVEL_SCRATCH = (
    "w", "deg", "own", "slot", "g", "gi", "x", "vb",
    "lo0", "lo1", "lo2", "lo3", "hi0", "hi1", "hi2", "hi3", "res", "oh",
    "rout", "rin", "rown", "uout", "uin",
)


def kernel(sizes, rhs_count, bs, k, coarse_all, *refs):
    refs = list(refs)
    take = lambda count: [refs.pop(0) for _ in range(count)]
    rhs_hbm, inverse_hbm = take(2)
    columns, hbm = [], []
    for _ in sizes:
        columns.append(refs.pop(0))
        hbm.append(dict(zip(LEVEL_HBM, take(4))))
    (out_hbm,) = take(1)
    scratch = [dict(zip(LEVEL_SCRATCH, take(len(LEVEL_SCRATCH)))) for _ in sizes]
    rhs, f_second, f_third, inverse, gathered, out = take(6)
    send, recv, gather_send, gather_recv, local, out_sem = take(6)

    ops = Ops(send, recv)
    levels = []
    for position, (n, t) in enumerate(sizes):
        ref = scratch[position]
        ref["sem"] = position * 6
        ref["f"] = (rhs, f_second, f_third)[position]
        levels.append(Level(n, t, rhs_count, bs, k, ref, hbm[position], columns[position], ops))
    fine, second, third = levels

    loads = []

    def load(src, dst):
        copy = pltpu.make_async_copy(src, dst, local.at[len(loads)])
        loads.append(copy)
        copy.start()
        return copy

    n = fine.n
    early = []
    for at in (slice(0, 2), slice(n - 2, n)):
        early.append(load(hbm[0]["w"].at[at], scratch[0]["w"].at[at]))
    early.append(load(hbm[0]["deg"], scratch[0]["deg"]))
    early.append(load(rhs_hbm, rhs))
    middle = load(hbm[0]["w"].at[2 : n - 2], scratch[0]["w"].at[2 : n - 2])
    later = [
        load(hbm[0][name], scratch[0][name]) for name in ("own", "slot")
    ]
    for position in (1, 2):
        later += [load(hbm[position][name], scratch[position][name]) for name in LEVEL_HBM]
    later.append(load(inverse_hbm, inverse))

    barrier = pltpu.get_barrier_semaphore()
    next_row = jnp.logical_and(ops.has_right, ops.col == ops.cols - 1)
    previous_row = jnp.logical_and(ops.has_left, ops.col == 0)
    pl.when(next_row)(
        lambda: pl.semaphore_signal(barrier, inc=1, device_id=ops.right, device_id_type=MESH)
    )
    pl.when(previous_row)(
        lambda: pl.semaphore_signal(barrier, inc=1, device_id=ops.left, device_id_type=MESH)
    )
    for step in range(1, ops.cols):
        peer = lax.rem(ops.col + step, ops.cols)
        pl.semaphore_signal(barrier, inc=1, device_id=(ops.row, peer), device_id_type=MESH)
    for level in levels:
        level.clear_ends()
    for copy in early:
        copy.wait()
    for b in fine.edges():
        fine.make_diagonal(b)
        fine.start_block(b)
    pl.semaphore_wait(
        barrier, ops.cols - 1 + next_row.astype(jnp.int32) + previous_row.astype(jnp.int32)
    )

    def middle_diagonal(b):
        fine.make_diagonal(b)

    fine.ops.start(fine.halo_copies(0))
    middle.wait()

    def inner_start(b):
        fine.make_diagonal(b)
        fine.start_block(b)

    loop(*fine.inner(), inner_start)
    for copy in later:
        copy.wait()
    loop(0, fine.n // 2, fine.make_onehot, 1)
    fine.apply(0, fine.first_sweep)
    fine.ops.start(fine.halo_copies(1))
    loop(fine.n // 2, fine.n, fine.make_onehot, 1)
    for level in (second, third):
        loop(0, level.n, level.make_onehot, 1)
        loop(0, level.n, level.make_diagonal, 4)
    fine.apply(1, fine.residual)

    def into_level(level):
        def into(block, value):
            level.ref["f"][block] = value

        return into

    fine.restrict(into_level(second))
    for level, following in ((second, third), (third, None)):
        for b in level.edges():
            level.start_block(b)
        if following is not None:
            level.down(into_level(following))
        else:

            def into_coarse(block, value):
                gathered[ops.col] = value.astype(BF16)

            level.down(into_coarse)

    sends = []
    for step in range(1, ops.cols):
        peer = lax.rem(ops.col + step, ops.cols)
        copy = pltpu.make_async_remote_copy(
            gathered.at[ops.col], gathered.at[ops.col],
            gather_send.at[step - 1], gather_recv.at[step - 1],
            device_id=(ops.row, peer), device_id_type=MESH,
        )
        copy.start()
        sends.append(copy)
    for step in range(1, ops.cols):
        source = lax.rem(ops.col + ops.cols - step, ops.cols)
        pltpu.make_async_remote_copy(
            gathered.at[source], gathered.at[source],
            gather_send.at[step - 1], gather_recv.at[step - 1],
            device_id=(ops.row, source), device_id_type=MESH,
        ).wait_recv()
    everything = jnp.concatenate([gathered[p] for p in range(ops.cols)], axis=1)
    solved = lax.dot_general(
        everything, inverse[...], (((1,), (1,)), ((), ())), preferred_element_type=F32
    )
    third.ref["uout"][...] = solved.astype(BF16)

    def into_coarse_vector(level):
        def put(b, x):
            level.ref["uout"][:, b * bs : (b + 1) * bs] = x.astype(BF16)

        return put

    third.up(into_coarse_vector(second))
    second.up(into_coarse_vector(fine))

    def put_out(b, x):
        out[b] = x

    fine.up(put_out)
    result = pltpu.make_async_copy(out, out_hbm, out_sem.at[0])
    result.start()
    for level in levels:
        level.drain()
    for copy in sends:
        copy.wait_send()
    result.wait()


def on_device(
    right_sides,
    weights_fine, columns_fine, degree_fine, owners_fine, slots_fine,
    weights_second, columns_second, degree_second, owners_second, slots_second,
    weights_third, columns_third, degree_third, owners_third, slots_third,
    coarse_inverse,
):
    n0, r, bs = right_sides.shape
    n1, n2 = weights_second.shape[0], weights_third.shape[0]
    k = weights_fine.shape[1]
    c3, m3 = coarse_inverse.shape
    cols = lax.axis_size("col")
    sizes = ((n0, n1 * bs), (n1, n2 * bs), (n2, c3))
    merged = lambda w: w.reshape(w.shape[0], k * bs, bs)
    args = [right_sides, coarse_inverse]
    specs = [pl.BlockSpec(memory_space=pl.ANY)] * 2
    for w, c, d, o, s in (
        (weights_fine, columns_fine, degree_fine, owners_fine, slots_fine),
        (weights_second, columns_second, degree_second, owners_second, slots_second),
        (weights_third, columns_third, degree_third, owners_third, slots_third),
    ):
        args += [c, merged(w), d, o, s]
        specs += [pl.BlockSpec(memory_space=pltpu.SMEM)]
        specs += [pl.BlockSpec(memory_space=pl.ANY)] * 4
    scratch = []
    for n, t in sizes:
        scratch += [
            pltpu.VMEM((n, k * bs, bs), BF16),
            pltpu.VMEM((n, bs), F32),
            pltpu.VMEM((n, bs), jnp.int32),
            pltpu.VMEM((n, bs), jnp.int32),
            pltpu.VMEM((n, 8, bs), F32),
            pltpu.VMEM((n, 8, bs), F32),
            pltpu.VMEM((n, r, bs), F32),
            pltpu.VMEM((4, n, r, bs), BF16),
            *[pltpu.VMEM((6, r, bs), BF16)] * 8,
            pltpu.VMEM(((4 if SPLIT_OWN else 3) * r, n * bs), BF16),
            pltpu.VMEM((t, n * bs), BF16),
            pltpu.VMEM((2, r, t), BF16),
            pltpu.VMEM((2, r, t), BF16),
            pltpu.VMEM((r, t), F32),
            pltpu.VMEM((r, t), BF16),
            pltpu.VMEM((2, r, t), BF16),
        ]
    scratch += [
        pltpu.VMEM((n0, r, bs), BF16),
        pltpu.VMEM((n1, r, bs), F32),
        pltpu.VMEM((n2, r, bs), F32),
        pltpu.VMEM((c3, m3), BF16),
        pltpu.VMEM((cols, r, c3), BF16),
        pltpu.VMEM((n0, r, bs), F32),
        pltpu.SemaphoreType.DMA((18, 2)),
        pltpu.SemaphoreType.DMA((18, 2)),
        pltpu.SemaphoreType.DMA((cols,)),
        pltpu.SemaphoreType.DMA((cols,)),
        pltpu.SemaphoreType.DMA((24,)),
        pltpu.SemaphoreType.DMA((1,)),
    ]
    return pl.pallas_call(
        functools.partial(kernel, sizes, r, bs, k, m3),
        out_shape=jax.ShapeDtypeStruct((n0, r, bs), F32),
        in_specs=specs,
        out_specs=pl.BlockSpec(memory_space=pl.ANY),
        scratch_shapes=scratch,
        compiler_params=pltpu.CompilerParams(
            collective_id=0, has_side_effects=True, vmem_limit_bytes=48 * 1024 * 1024
        ),
        name="vcycle",
    )(*args)


def solution(mesh):
    whole = ("row", "col")
    vector, matrix, table = P(whole, None, None), P(whole, None, None, None), P(whole, None)
    level = (matrix, table, table, table, table)
    return jax.shard_map(
        on_device,
        mesh=mesh,
        in_specs=(vector, *level, *level, *level, table),
        out_specs=vector,
        check_vma=False,
    )
```

```python
import functools

import jax
import jax.numpy as jnp
from jax import lax
from jax.experimental import pallas as pl
from jax.experimental.pallas import tpu as pltpu
from jax.sharding import PartitionSpec as P

F32 = jnp.float32
BF16 = jnp.bfloat16
MESH = pl.DeviceIdType.MESH
DAMPING = 0.8
SPLIT_OWN = False


def loop(low, high, body, unroll=4):
    count = high - low
    if count <= 0:
        return
    while count % unroll:
        unroll -= 1

    if count == unroll:
        for inner in range(count):
            body(low + inner)
        return

    def step(outer, carry):
        for inner in range(unroll):
            body(low + outer * unroll + inner)
        return carry

    lax.fori_loop(0, count // unroll, step, 0)


def grouped(low, high, first, then, unroll=7):
    count = high - low
    if count <= 0:
        return
    while count % unroll:
        unroll -= 1

    def group(start):
        made = [first(start + inner) for inner in range(unroll)]
        for inner in range(unroll):
            then(start + inner, made[inner])

    if count == unroll:
        group(low)
        return

    def step(outer, carry):
        group(low + outer * unroll)
        return carry

    lax.fori_loop(0, count // unroll, step, 0)


class Level:
    def __init__(self, blocks, coarse, rhs_count, bs, k, ref, hbm, columns, ops):
        self.n, self.t, self.r, self.bs, self.k = blocks, coarse, rhs_count, bs, k
        self.ref, self.hbm, self.columns, self.ops = ref, hbm, columns, ops
        self.single = blocks < 4
        self.base = ops.me * blocks
        self.scale = 1.0 / (k * bs)

    def edges(self):
        n = self.n
        if self.single:
            return list(range(n))
        return [0, 1, n - 2, n - 1]

    def inner(self):
        return (0, 0) if self.single else (2, self.n - 2)

    def weight_sums(self, b):
        w = self.ref["w"][b]
        return jnp.dot(jnp.ones((8, w.shape[0]), BF16), w, preferred_element_type=F32)

    def put_diagonal(self, b, total):
        degree = self.ref["deg"][pl.ds(b, 1), :]
        g = degree + total * self.scale
        self.ref["g"][b] = g
        self.ref["gi"][b] = DAMPING / g

    def row(self, name, b):
        value = self.ref[name][b, 0:1, :]
        return jnp.broadcast_to(value, (self.r, self.bs))

    def f(self, b):
        return self.ref["f"][b].astype(F32)

    def product(self, i, b, where):
        if where == "inner":
            buf, offset = self.ref[f"vb{i}"], self.base
        elif where == "low":
            buf, offset = self.ref[f"lo{i}"], self.base - 2
        else:
            buf, offset = self.ref[f"hi{i}"], self.base + self.n - 4
        top = buf.shape[0] - 1
        picked = [
            buf[jnp.clip(self.columns[b, k] - offset, 0, top)] for k in range(self.k)
        ]
        left = jnp.concatenate(picked, axis=1)
        return jnp.dot(left, self.ref["w"][b], preferred_element_type=F32) * self.scale

    def halo_copies(self, i):
        n, ops, vb = self.n, self.ops, self.ref[f"vb{i}"]
        if self.single:
            low_dst, high_dst = self.ref[f"lo{i}"].at[0:2], self.ref[f"lo{i}"].at[4:6]
        else:
            low_dst, high_dst = self.ref[f"lo{i}"].at[0:2], self.ref[f"hi{i}"].at[4:6]
        return ops.pair(vb.at[n - 2 : n], low_dst, vb.at[0:2], high_dst, self.ref["sem"] + i)

    def fill_edges(self, i):
        n = self.n
        if self.single:
            self.ref[f"lo{i}"][2:4] = self.ref[f"vb{i}"][0:2]
        else:
            self.ref[f"lo{i}"][2:6] = self.ref[f"vb{i}"][0:4]
            self.ref[f"hi{i}"][0:4] = self.ref[f"vb{i}"][n - 4 : n]

    def run_edges(self, i, body):
        made = [self.product(i, b, "low" if b < 2 else "high") for b in self.edges()]
        for b, product in zip(self.edges(), made):
            body(b, product)

    def apply(self, i, body):
        grouped(*self.inner(), lambda b: self.product(i, b, "inner"), body)
        self.fill_edges(i)
        self.ops.wait(self.halo_copies(i))
        self.run_edges(i, body)

    def start_block(self, b):
        self.ref["vb0"][b] = (self.row("gi", b) * self.f(b)).astype(BF16)

    def first_sweep(self, b, product):
        f, gi = self.f(b), self.row("gi", b)
        x0 = gi * f
        x = (1.0 - DAMPING) * x0 + gi * (f + product)
        self.ref["x"][b] = x
        self.ref["vb1"][b] = x.astype(BF16)

    def residual(self, b, product):
        res = self.f(b) - self.row("g", b) * self.ref["x"][b] + product
        rel = self.owner(b)
        columns = pl.ds(pl.multiple_of(b * self.bs, self.bs), self.bs)
        rows = self.r
        high = res.astype(BF16)
        zero = jnp.zeros_like(res)
        out = self.ref["res"]
        out[0:rows, columns] = jnp.where(rel < 0, res, zero).astype(BF16)
        out[rows : 2 * rows, columns] = jnp.where(rel > 0, res, zero).astype(BF16)
        own = jnp.where(rel == 0, res, zero)
        high = own.astype(BF16)
        out[2 * rows : 3 * rows, columns] = high
        if SPLIT_OWN:
            out[3 * rows : 4 * rows, columns] = (own - high.astype(F32)).astype(BF16)

    def owner(self, b):
        value = self.ref["own"][pl.ds(b, 1), :] - self.ops.me
        return jnp.broadcast_to(value, (self.r, self.bs))

    def make_onehot(self, b):
        columns = pl.ds(pl.multiple_of(b * self.bs, self.bs), self.bs)
        slots = jnp.broadcast_to(self.ref["slot"][pl.ds(b, 1), :], (self.t, self.bs))
        index = lax.broadcasted_iota(jnp.int32, (self.t, self.bs), 0)
        self.ref["oh"][:, columns] = jnp.where(index == slots, 1.0, 0.0).astype(BF16)

    def restricted(self, rows, put):
        tile = min(self.t, 256)

        def body(j):
            at = pl.ds(pl.multiple_of(j * tile, tile), tile)
            put(
                at,
                lax.dot_general(
                    self.ref["res"][rows, :],
                    self.ref["oh"][at, :],
                    (((1,), (1,)), ((), ())),
                    preferred_element_type=F32,
                ),
            )

        loop(0, self.t // tile, body, 1)

    def restrict_copies(self):
        out, got = self.ref["rout"], self.ref["rin"]
        return self.ops.pair(out.at[1], got.at[0], out.at[0], got.at[1], self.ref["sem"] + 4)

    def restrict(self, into):
        r = self.r

        def put_out(at, value):
            self.ref["rout"][0, :, at] = value[0:r].astype(BF16)
            self.ref["rout"][1, :, at] = value[r : 2 * r].astype(BF16)

        self.restricted(slice(0, 2 * r), put_out)
        copies = self.restrict_copies()
        self.ops.start(copies)

        def put_own(at, value):
            if SPLIT_OWN:
                value = value[0:r] + value[r : 2 * r]
            self.ref["rown"][:, at] = value

        self.restricted(slice(2 * r, (4 if SPLIT_OWN else 3) * r), put_own)
        self.ops.wait(copies)
        for block in range(self.t // self.bs):
            at = slice(block * self.bs, (block + 1) * self.bs)
            into(
                block,
                self.ref["rown"][:, at]
                + self.ref["rin"][0, :, at].astype(F32)
                + self.ref["rin"][1, :, at].astype(F32),
            )

    def down(self, into, while_first=None, while_second=None):
        self.ops.start(self.halo_copies(0))
        loop(*self.inner(), self.start_block)
        if while_first is not None:
            while_first()
        self.apply(0, self.first_sweep)
        self.ops.start(self.halo_copies(1))
        if while_second is not None:
            while_second()
        self.apply(1, self.residual)
        self.restrict(into)

    def prolong_copies(self):
        out, got = self.ref["uout"], self.ref["uin"]
        return self.ops.pair(out, got.at[0], out, got.at[1], self.ref["sem"] + 5)

    def pair_columns(self, pair):
        return pl.ds(pl.multiple_of(pair * 2 * self.bs, 2 * self.bs), 2 * self.bs)

    def own_part(self, pair):
        return jnp.dot(
            self.ref["uout"][...], self.ref["oh"][:, self.pair_columns(pair)],
            preferred_element_type=F32,
        )

    def add_own(self, pair, value):
        for half in range(2):
            b = 2 * pair + half
            part = value[:, half * self.bs : (half + 1) * self.bs]
            self.ref["x"][b] = self.ref["x"][b] + jnp.where(self.owner(b) == 0, part, 0.0)

    def others_part(self, pair):
        left = jnp.concatenate([self.ref["uin"][0], self.ref["uin"][1]], axis=0)
        return jnp.dot(
            left, self.ref["oh"][:, self.pair_columns(pair)], preferred_element_type=F32
        )

    def add_others(self, pair, value):
        for half in range(2):
            b = 2 * pair + half
            at = slice(half * self.bs, (half + 1) * self.bs)
            rel = self.owner(b)
            x = self.ref["x"][b]
            x = x + jnp.where(rel < 0, value[0 : self.r, at], 0.0)
            x = x + jnp.where(rel > 0, value[self.r : 2 * self.r, at], 0.0)
            self.ref["x"][b] = x
            self.ref["vb2"][b] = x.astype(BF16)

    def sweep(self, i, last, out=None):
        def body(b, product):
            gi = self.row("gi", b)
            x = (1.0 - DAMPING) * self.ref["x"][b] + gi * (self.f(b) + product)
            self.ref["x"][b] = x
            if not last:
                self.ref[f"vb{i + 1}"][b] = x.astype(BF16)
            elif out is not None:
                out(b, x)

        return body

    def up(self, out=None):
        copies = self.prolong_copies()
        self.ops.start(copies)
        pairs = self.n // 2
        grouped(0, pairs, self.own_part, self.add_own, 2)
        self.ops.wait(copies)
        ends = [0] if self.single else [0, pairs - 1]
        made = [self.others_part(pair) for pair in ends]
        for pair, value in zip(ends, made):
            self.add_others(pair, value)
        self.ops.start(self.halo_copies(2))
        if not self.single:
            grouped(1, pairs - 1, self.others_part, self.add_others, 2)
        self.apply(2, self.sweep(2, False))
        self.ops.start(self.halo_copies(3))
        self.apply(3, self.sweep(3, True, out))

    def drain(self):
        for i in range(4):
            self.ops.drain(self.halo_copies(i))
        self.ops.drain(self.restrict_copies())
        self.ops.drain(self.prolong_copies())

    def clear_ends(self):
        for name, first, last in (("rin", 0, 1), ("uin", 0, 1)):
            ref = self.ref[name]

            @pl.when(self.ops.me == 0)
            def _():
                ref[first] = jnp.zeros(ref.shape[1:], ref.dtype)

            @pl.when(self.ops.me == self.ops.total - 1)
            def _():
                ref[last] = jnp.zeros(ref.shape[1:], ref.dtype)


class Ops:
    def __init__(self, send, recv):
        self.send, self.recv = send, recv
        self.rows, self.cols = lax.axis_size("row"), lax.axis_size("col")
        self.total = self.rows * self.cols
        self.row, self.col = lax.axis_index("row"), lax.axis_index("col")
        self.me = self.row * self.cols + self.col
        right = jnp.minimum(self.me + 1, self.total - 1)
        left = jnp.maximum(self.me - 1, 0)
        self.right = (right // self.cols, right % self.cols)
        self.left = (left // self.cols, left % self.cols)
        self.has_right = self.me < self.total - 1
        self.has_left = self.me > 0

    def pair(self, to_right, at_right, to_left, at_left, slot):
        first = pltpu.make_async_remote_copy(
            to_right, at_right, self.send.at[slot, 0], self.recv.at[slot, 0],
            device_id=self.right, device_id_type=MESH,
        )
        second = pltpu.make_async_remote_copy(
            to_left, at_left, self.send.at[slot, 1], self.recv.at[slot, 1],
            device_id=self.left, device_id_type=MESH,
        )
        return first, second

    def start(self, copies):
        pl.when(self.has_right)(lambda: copies[0].start())
        pl.when(self.has_left)(lambda: copies[1].start())

    def wait(self, copies):
        pl.when(self.has_left)(lambda: copies[0].wait_recv())
        pl.when(self.has_right)(lambda: copies[1].wait_recv())

    def drain(self, copies):
        pl.when(self.has_right)(lambda: copies[0].wait_send())
        pl.when(self.has_left)(lambda: copies[1].wait_send())


LEVEL_HBM = ("w", "deg", "own", "slot")
LEVEL_SCRATCH = (
    "w", "deg", "own", "slot", "g", "gi", "x", "vb0", "vb1", "vb2", "vb3",
    "lo0", "lo1", "lo2", "lo3", "hi0", "hi1", "hi2", "hi3", "res", "oh",
    "rout", "rin", "rown", "uout", "uin",
)


def kernel(sizes, rhs_count, bs, k, coarse_all, *refs):
    refs = list(refs)
    take = lambda count: [refs.pop(0) for _ in range(count)]
    rhs_hbm, inverse_hbm = take(2)
    columns, hbm = [], []
    for _ in sizes:
        columns.append(refs.pop(0))
        hbm.append(dict(zip(LEVEL_HBM, take(4))))
    (out_hbm,) = take(1)
    scratch = [dict(zip(LEVEL_SCRATCH, take(len(LEVEL_SCRATCH)))) for _ in sizes]
    rhs, f_second, f_third, inverse, gathered, out = take(6)
    send, recv, gather_send, gather_recv, local, out_sem = take(6)

    ops = Ops(send, recv)
    levels = []
    for position, (n, t) in enumerate(sizes):
        ref = scratch[position]
        ref["sem"] = position * 6
        ref["f"] = (rhs, f_second, f_third)[position]
        levels.append(Level(n, t, rhs_count, bs, k, ref, hbm[position], columns[position], ops))
    fine, second, third = levels

    loads = []

    def load(src, dst):
        copy = pltpu.make_async_copy(src, dst, local.at[len(loads)])
        loads.append(copy)
        copy.start()
        return copy

    n = fine.n
    early = []
    for at in (slice(0, 2), slice(n - 2, n)):
        early.append(load(hbm[0]["w"].at[at], scratch[0]["w"].at[at]))
    early.append(load(hbm[0]["deg"], scratch[0]["deg"]))
    early.append(load(rhs_hbm, rhs))
    middle = load(hbm[0]["w"].at[2 : n - 2], scratch[0]["w"].at[2 : n - 2])
    later = [
        load(hbm[0][name], scratch[0][name]) for name in ("own", "slot")
    ]
    for position in (1, 2):
        later += [load(hbm[position][name], scratch[position][name]) for name in LEVEL_HBM]
    later.append(load(inverse_hbm, inverse))

    barrier = pltpu.get_barrier_semaphore()
    next_row = jnp.logical_and(ops.has_right, ops.col == ops.cols - 1)
    previous_row = jnp.logical_and(ops.has_left, ops.col == 0)
    pl.when(next_row)(
        lambda: pl.semaphore_signal(barrier, inc=1, device_id=ops.right, device_id_type=MESH)
    )
    pl.when(previous_row)(
        lambda: pl.semaphore_signal(barrier, inc=1, device_id=ops.left, device_id_type=MESH)
    )
    for step in range(1, ops.cols):
        peer = lax.rem(ops.col + step, ops.cols)
        pl.semaphore_signal(barrier, inc=1, device_id=(ops.row, peer), device_id_type=MESH)
    for level in levels:
        level.clear_ends()
    for copy in early:
        copy.wait()
    def diagonal_and_start(b, total):
        fine.put_diagonal(b, total)
        fine.start_block(b)

    made = [fine.weight_sums(b) for b in fine.edges()]
    for b, total in zip(fine.edges(), made):
        diagonal_and_start(b, total)
    pl.semaphore_wait(
        barrier, ops.cols - 1 + next_row.astype(jnp.int32) + previous_row.astype(jnp.int32)
    )

    fine.ops.start(fine.halo_copies(0))
    middle.wait()

    grouped(*fine.inner(), fine.weight_sums, diagonal_and_start)
    for copy in later:
        copy.wait()
    loop(0, fine.n // 2, fine.make_onehot, 1)
    fine.apply(0, fine.first_sweep)
    fine.ops.start(fine.halo_copies(1))
    loop(fine.n // 2, fine.n, fine.make_onehot, 1)
    for level in (second, third):
        loop(0, level.n, level.make_onehot, 1)
        grouped(0, level.n, level.weight_sums, level.put_diagonal, 8)
    fine.apply(1, fine.residual)

    def into_level(level):
        def into(block, value):
            level.ref["f"][block] = value

        return into

    fine.restrict(into_level(second))
    for level, following in ((second, third), (third, None)):
        for b in level.edges():
            level.start_block(b)
        if following is not None:
            level.down(into_level(following))
        else:

            def into_coarse(block, value):
                gathered[ops.col] = value.astype(BF16)

            level.down(into_coarse)

    sends = []
    for step in range(1, ops.cols):
        peer = lax.rem(ops.col + step, ops.cols)
        copy = pltpu.make_async_remote_copy(
            gathered.at[ops.col], gathered.at[ops.col],
            gather_send.at[step - 1], gather_recv.at[step - 1],
            device_id=(ops.row, peer), device_id_type=MESH,
        )
        copy.start()
        sends.append(copy)
    for step in range(1, ops.cols):
        source = lax.rem(ops.col + ops.cols - step, ops.cols)
        pltpu.make_async_remote_copy(
            gathered.at[source], gathered.at[source],
            gather_send.at[step - 1], gather_recv.at[step - 1],
            device_id=(ops.row, source), device_id_type=MESH,
        ).wait_recv()
    everything = jnp.concatenate([gathered[p] for p in range(ops.cols)], axis=1)
    solved = lax.dot_general(
        everything, inverse[...], (((1,), (1,)), ((), ())), preferred_element_type=F32
    )
    third.ref["uout"][...] = solved.astype(BF16)

    def into_coarse_vector(level):
        def put(b, x):
            level.ref["uout"][:, b * bs : (b + 1) * bs] = x.astype(BF16)

        return put

    third.up(into_coarse_vector(second))
    second.up(into_coarse_vector(fine))

    def put_out(b, x):
        out[b] = x

    fine.up(put_out)
    result = pltpu.make_async_copy(out, out_hbm, out_sem.at[0])
    result.start()
    for level in levels:
        level.drain()
    for copy in sends:
        copy.wait_send()
    result.wait()


def on_device(
    right_sides,
    weights_fine, columns_fine, degree_fine, owners_fine, slots_fine,
    weights_second, columns_second, degree_second, owners_second, slots_second,
    weights_third, columns_third, degree_third, owners_third, slots_third,
    coarse_inverse,
):
    n0, r, bs = right_sides.shape
    n1, n2 = weights_second.shape[0], weights_third.shape[0]
    k = weights_fine.shape[1]
    c3, m3 = coarse_inverse.shape
    cols = lax.axis_size("col")
    sizes = ((n0, n1 * bs), (n1, n2 * bs), (n2, c3))
    merged = lambda w: w.reshape(w.shape[0], k * bs, bs)
    args = [right_sides, coarse_inverse]
    specs = [pl.BlockSpec(memory_space=pl.ANY)] * 2
    for w, c, d, o, s in (
        (weights_fine, columns_fine, degree_fine, owners_fine, slots_fine),
        (weights_second, columns_second, degree_second, owners_second, slots_second),
        (weights_third, columns_third, degree_third, owners_third, slots_third),
    ):
        args += [c, merged(w), d, o, s]
        specs += [pl.BlockSpec(memory_space=pltpu.SMEM)]
        specs += [pl.BlockSpec(memory_space=pl.ANY)] * 4
    scratch = []
    for n, t in sizes:
        scratch += [
            pltpu.VMEM((n, k * bs, bs), BF16),
            pltpu.VMEM((n, bs), F32),
            pltpu.VMEM((n, bs), jnp.int32),
            pltpu.VMEM((n, bs), jnp.int32),
            pltpu.VMEM((n, 8, bs), F32),
            pltpu.VMEM((n, 8, bs), F32),
            pltpu.VMEM((n, r, bs), F32),
            *[pltpu.VMEM((n, r, bs), BF16)] * 4,
            *[pltpu.VMEM((6, r, bs), BF16)] * 8,
            pltpu.VMEM(((4 if SPLIT_OWN else 3) * r, n * bs), BF16),
            pltpu.VMEM((t, n * bs), BF16),
            pltpu.VMEM((2, r, t), BF16),
            pltpu.VMEM((2, r, t), BF16),
            pltpu.VMEM((r, t), F32),
            pltpu.VMEM((r, t), BF16),
            pltpu.VMEM((2, r, t), BF16),
        ]
    scratch += [
        pltpu.VMEM((n0, r, bs), BF16),
        pltpu.VMEM((n1, r, bs), F32),
        pltpu.VMEM((n2, r, bs), F32),
        pltpu.VMEM((c3, m3), BF16),
        pltpu.VMEM((cols, r, c3), BF16),
        pltpu.VMEM((n0, r, bs), F32),
        pltpu.SemaphoreType.DMA((18, 2)),
        pltpu.SemaphoreType.DMA((18, 2)),
        pltpu.SemaphoreType.DMA((cols,)),
        pltpu.SemaphoreType.DMA((cols,)),
        pltpu.SemaphoreType.DMA((24,)),
        pltpu.SemaphoreType.DMA((1,)),
    ]
    return pl.pallas_call(
        functools.partial(kernel, sizes, r, bs, k, m3),
        out_shape=jax.ShapeDtypeStruct((n0, r, bs), F32),
        in_specs=specs,
        out_specs=pl.BlockSpec(memory_space=pl.ANY),
        scratch_shapes=scratch,
        compiler_params=pltpu.CompilerParams(
            collective_id=0, has_side_effects=True, vmem_limit_bytes=48 * 1024 * 1024
        ),
        name="vcycle",
    )(*args)


def solution(mesh):
    whole = ("row", "col")
    vector, matrix, table = P(whole, None, None), P(whole, None, None, None), P(whole, None)
    level = (matrix, table, table, table, table)
    return jax.shard_map(
        on_device,
        mesh=mesh,
        in_specs=(vector, *level, *level, *level, table),
        out_specs=vector,
        check_vma=False,
    )
```
